128 devices in a mesh: dp: 4 (over y_hi, core), tp: 32 (over y_lo, x, z).
Axes of the slice: x: 4, y: 4 (y_hi: 2, y_lo: 2; y = y_hi * 2 + y_lo), z: 4, core: 2. Of those that a mesh axis runs over, the one named last changes fastest.
Arguments:
- tokens: bfloat16 [1024, 7168], P(('dp', 'tp')), may hold values from -6 to 6
- w_gate: bfloat16 [7168, 12288], P(None, 'tp'), may hold values from -0.0625 to 0.0625
- w_up: bfloat16 [7168, 12288], P(None, 'tp'), may hold values from -0.0625 to 0.0625
- w_down: bfloat16 [12288, 7168], P('tp'), may hold values from -0.0546875 to 0.0546875
- cotangent: bfloat16 [1024, 7168], P(('dp', 'tp')), may hold values from -6 to 6
Outputs:
- mixed: bfloat16 [1024, 7168], P(('dp', 'tp'))
- input_grad: bfloat16 [1024, 7168], P(('dp', 'tp'))
- gate_grad: float32 [7168, 12288], P('dp', 'tp')
- up_grad: float32 [7168, 12288], P('dp', 'tp')
- down_grad: float32 [12288, 7168], P('tp', 'dp')
The draws below stay inside these ranges and needn't reach their ends.
All inputs are finite; a program needn't handle non-finite values.
Results may differ from the reference program's by a relative error of at most 0.0049.
Values may be sent and summed in bfloat16 or wider, within the bound.
A program may use at most 192 MiB of HBM per device.

```python
import jax
import jax.numpy as jnp

D = 7168
FF = 12288
TOKENS = 1024


def shard_levels(key, shape, cuts, low, largest):
    def one(dim, parts):
        steps = jax.random.uniform(jax.random.fold_in(jax.random.fold_in(key, 6), dim), (parts,), jnp.float32, low / len(cuts), largest / len(cuts))
        return jnp.repeat(jnp.exp(steps), shape[dim] // parts).reshape((-1,) + (1,) * (len(shape) - dim - 1))

    loudness = one(*cuts[0])
    for cut in cuts[1:]:
        loudness = loudness * one(*cut)
    return loudness


def gaussian(own_key, extent, scale, reach, cuts=(), held_as=jnp.bfloat16):
    loudness = shard_levels(own_key, extent, cuts, -0.22, 0.18) if cuts else 1.0
    drawn = jax.random.normal(own_key, extent, jnp.float32) * scale * loudness
    return jnp.minimum(jnp.maximum(drawn, -reach), reach).astype(held_as)


def setup_inputs(seed: int = 0) -> dict:
    arg_keys = jax.random.split(jax.random.key(seed), 6)
    return {
        "tokens": gaussian(arg_keys[0], (TOKENS, D), 1.0, 6.0, ((0, 128),)),
        "w_gate": gaussian(arg_keys[1], (D, FF), D ** -0.5, 0.0625, ((1, 32),)),
        "w_up": gaussian(arg_keys[2], (D, FF), D ** -0.5, 0.0625, ((1, 32),)),
        "w_down": gaussian(arg_keys[3], (FF, D), FF ** -0.5, 0.0546875, ((0, 32),)),
        "cotangent": gaussian(arg_keys[4], (TOKENS, D), 1.0, 6.0, ((0, 128),)),
    }


def reference(tokens, w_gate, w_up, w_down, cotangent):
    gate = jnp.dot(tokens, w_gate, preferred_element_type=jnp.float32)
    up = jnp.dot(tokens, w_up, preferred_element_type=jnp.float32)
    sig = jax.nn.sigmoid(gate)
    act = gate * sig
    hidden = (act * up).astype(jnp.bfloat16)
    mixed = jnp.dot(hidden, w_down, preferred_element_type=jnp.float32).astype(jnp.bfloat16)
    back = jnp.dot(cotangent, w_down.T, preferred_element_type=jnp.float32)
    dgate = (back * up * sig * (1.0 + gate * (1.0 - sig))).astype(jnp.bfloat16)
    dup = (back * act).astype(jnp.bfloat16)
    input_grad = (jnp.dot(dgate, w_gate.T, preferred_element_type=jnp.float32)
                  + jnp.dot(dup, w_up.T, preferred_element_type=jnp.float32)).astype(jnp.bfloat16)
    gate_grad = jnp.dot(tokens.T, dgate, preferred_element_type=jnp.float32)
    up_grad = jnp.dot(tokens.T, dup, preferred_element_type=jnp.float32)
    down_grad = jnp.dot(hidden.T, cotangent, preferred_element_type=jnp.float32)
    return mixed, input_grad, gate_grad, up_grad, down_grad
```

```python
import functools

import jax
import jax.numpy as jnp
from jax import lax
from jax.experimental import pallas as pl
from jax.experimental.pallas import tpu as pltpu
from jax.sharding import Mesh
from jax.sharding import PartitionSpec as P

TP = ("yl", "x", "z")
DP = ("yh", "co")
DP_TP = DP + TP
BF = jnp.bfloat16
F32 = jnp.float32

D = 7168
DB = 1792
H = 384
T = 1024
CH = 256
HC = 128

KIDS = {0: ((1, 1), (3, -1)), 1: ((2, 1),), 2: (), 3: ()}
IJ = (
    (0, 0),
    (1, 0), (0, 1), (3, 0), (0, 3),
    (2, 0), (1, 1), (3, 1), (1, 3), (0, 2), (3, 3),
    (2, 1), (1, 2), (3, 2), (2, 3),
    (2, 2),
)
KEPT = tuple(ij for ij in IJ if ij[1] < 2)
OI = {ij: n for n, ij in enumerate(IJ)}


def kernel(
    tok_in, cot_in, wg, wu, wd,
    sgu, sdg, yor,
    tok, cot, yin, big, wgu, wdn, gf, rb, xs, rl, yr, bf, rbb, xsb, rlb, yrb,
    sa, sd, hid, dgu, par, keep, rin, yse,
    ysend, yrecv, gsend, grecv, wsem, d1s, d1r, e1s, e1r, e2s, e2r,
    d2s, d2r, rsend, rrecv, fsend, frecv,
):
    yh, co, yl = lax.axis_index("yh"), lax.axis_index("co"), lax.axis_index("yl")
    x, z = lax.axis_index("x"), lax.axis_index("z")
    y = yh * 2 + yl
    f = y * 2 + co
    d = yh * 2 + co

    def ring_dev(g):
        gy = g // 2
        return {"yh": gy // 2, "yl": gy % 2, "co": g % 2}

    def y_dev(k):
        gy = (y + k) % 4
        return {"yh": gy // 2, "yl": gy % 2}

    def xz_dev(c, axis, way):
        s = (1 - 2 * (c % 2)) * way
        o = c // 2
        on_x = (1 - o) if axis == 0 else o
        return {"x": (x + s * on_x + 4) % 4, "z": (z + s * (1 - on_x) + 4) % 4}

    other = {"co": 1 - co}

    def rc(src, dst, ss, rs, dev):
        return pltpu.make_async_remote_copy(
            src_ref=src, dst_ref=dst, send_sem=ss, recv_sem=rs,
            device_id=dev, device_id_type=pl.DeviceIdType.MESH,
        )

    def got(dst, rs):
        rc(dst, dst, rs, rs, other).wait_recv()

    def sent(src, ss):
        rc(src, src, ss, ss, other).wait_send()

    w_copies = (
        pltpu.make_async_copy(wg.at[pl.ds(d * DB, DB), :], wgu.at[:, pl.ds(0, H)], wsem.at[0]),
        pltpu.make_async_copy(wu.at[pl.ds(d * DB, DB), :], wgu.at[:, pl.ds(H, H)], wsem.at[1]),
        pltpu.make_async_copy(wd.at[:, pl.ds(d * DB, DB)], wdn, wsem.at[2]),
    )
    in_copies = (
        pltpu.make_async_copy(tok_in, tok, wsem.at[3]),
        pltpu.make_async_copy(cot_in, cot, wsem.at[4]),
    )
    for cp in in_copies + w_copies:
        cp.start()

    barrier = pltpu.get_barrier_semaphore()
    for dev in ({"x": (x + 1) % 4}, {"x": (x + 3) % 4}, {"z": (z + 1) % 4}, {"z": (z + 3) % 4}):
        pl.semaphore_signal(barrier, inc=1, device_id=dev, device_id_type=pl.DeviceIdType.MESH)
    for k in range(1, 8):
        pl.semaphore_signal(
            barrier, inc=1, device_id=ring_dev((f + k) % 8), device_id_type=pl.DeviceIdType.MESH
        )
    pl.semaphore_wait(barrier, 11)

    for a, src in ((0, tok), (1, cot)):
        in_copies[a].wait()

        @pl.loop(0, 7)
        def _(n):
            k = (n + 1) // 2
            g = ((y + k + (k // 2) * (1 - 2 * (k // 3))) % 4) * 2 + (co + n + 1) % 2
            gd = (g // 4) * 2 + g % 2
            rc(
                src.at[:, pl.ds(pl.multiple_of(gd * DB, 128), DB)], yin.at[a, f],
                ysend.at[a, g], yrecv.at[a, f], ring_dev(g),
            ).start()
    for a, src in ((0, tok), (1, cot)):
        yin[a, f] = src[:, pl.ds(pl.multiple_of(d * DB, 128), DB)]

    def rows(oi, c):
        return pl.ds(pl.multiple_of(oi * 64 + c * 16, 16), 16)

    def near(n):
        return (y + n + (n // 2) * (1 - 2 * (n // 3))) % 4

    def along_second(a, oi, c):
        i, j = IJ[oi]
        src = big.at[a, rows(oi, c)]
        for kid, way in KIDS[j]:
            to = OI[i, kid]
            rc(src, big.at[a, rows(to, c)], gsend.at[a, to, c], grecv.at[a, to, c],
               xz_dev(c, 1, way)).start()

    def gather_step(a, oi):
        i, j = IJ[oi]

        @pl.loop(0, 4)
        def _(n):
            if oi == 0:
                c = near(n)
                halves = []
                for h in range(2):
                    g = c * 2 + h

                    @pl.when(g != f)
                    def _():
                        got(yin.at[a, g], yrecv.at[a, g])

                    halves.append(yin[a, g].astype(F32))
                big[a, rows(0, c), :] = jnp.concatenate(halves, axis=0).astype(BF)
            else:
                c = n
                got(big.at[a, rows(oi, c)], grecv.at[a, oi, c])
            src = big.at[a, rows(oi, c)]
            if j == 0:
                for kid, way in KIDS[i]:
                    to = OI[kid, 0]
                    rc(src, big.at[a, rows(to, c)], gsend.at[a, to, c], grecv.at[a, to, c],
                       xz_dev(c, 0, way)).start()
            if oi:
                along_second(a, oi, c)

        if oi == 0:
            @pl.loop(0, 4)
            def _(n):
                along_second(a, oi, near(n))

    mine = HC * co
    theirs = HC - mine

    def half_rows(k, off):
        return pl.ds(pl.multiple_of(k * CH + off, HC), HC)

    part = ((gf, rb, xs, rl, yr), (bf, rbb, xsb, rlb, yrb))

    def product(a, k):
        full = part[a][0]
        left = big.at[a, pl.ds(k * CH, CH)]
        if a == 0:
            if k == 0:
                w_copies[0].wait()
                w_copies[1].wait()

            @pl.loop(0, 3)
            def _(n):
                cols = pl.ds(pl.multiple_of(n * 256, 256), 256)
                full[pl.ds(k * CH, CH), cols] = jnp.dot(
                    left[...], wgu[:, cols], preferred_element_type=F32
                )
        else:
            if k == 0:
                w_copies[2].wait()
            full[pl.ds(k * CH, CH), :] = lax.dot_general(
                left[...], wdn[...], (((1,), (1,)), ((), ())), preferred_element_type=F32
            )
        rc(full.at[half_rows(k, theirs)], part[a][1].at[k], d1s.at[a, k], d1r.at[a, k], other).start()

    def chip_sum(a, k):
        full, recv, out, relay, _ = part[a]
        got(recv.at[k], d1r.at[a, k])
        s = full[half_rows(k, mine), :] + recv[k]
        full[half_rows(k, mine), :] = s
        out[k] = s.astype(BF)
        for w, way in ((0, 1), (1, -1)):
            rc(out.at[k, pl.ds(w * 64, 64)], relay.at[k, w], e1s.at[a, k, w], e1r.at[a, k, w],
               y_dev(way + 4)).start()

    def relay_on(a, k):
        _, _, _, relay, recv = part[a]
        for w, way in ((0, 1), (1, -1)):
            got(relay.at[k, w], e1r.at[a, k, w])
            rc(relay.at[k, w], recv.at[k, pl.ds(w * 64, 64)], e2s.at[a, k, w], e2r.at[a, k, w],
               y_dev(way + 4)).start()

    def total(a, k, cols):
        full, _, _, _, recv = part[a]
        return full[half_rows(k, mine), cols] + recv[k, :, cols].astype(F32)

    def arrived(a, k):
        recv = part[a][4]
        for w in range(2):
            got(recv.at[k, pl.ds(w * 64, 64)], e2r.at[a, k, w])

    def forward_act(k):
        arrived(0, k)
        gate = total(0, k, pl.ds(0, H))
        up = total(0, k, pl.ds(H, H))
        sig = 1.0 / (1.0 + jnp.exp(-gate))
        act = gate * sig
        sa[pl.ds(k * HC, HC), :] = act
        sd[pl.ds(k * HC, HC), :] = up * sig * (1.0 + gate * (1.0 - sig))
        hid[half_rows(k, mine), :] = (act * up).astype(BF)
        rc(hid.at[half_rows(k, mine)], hid.at[half_rows(k, mine)], d2s.at[0, k], d2r.at[0, k], other).start()

    def backward_act(k):
        arrived(1, k)
        back = total(1, k, pl.ds(0, H))
        dgu[half_rows(k, mine), pl.ds(0, H)] = (back * sd[pl.ds(k * HC, HC), :]).astype(BF)
        dgu[half_rows(k, mine), pl.ds(H, H)] = (back * sa[pl.ds(k * HC, HC), :]).astype(BF)
        rc(dgu.at[half_rows(k, mine)], dgu.at[half_rows(k, mine)], d2s.at[1, k], d2r.at[1, k], other).start()

    def put(a, k, cols, r):
        for n in range(8):
            oi = 8 * k + n
            piece = r[n * 64 : n * 64 + 64]
            if IJ[oi] in KEPT:
                keep[a, pl.ds(KEPT.index(IJ[oi]) * 64, 64), cols] = piece
            else:
                par[a, pl.ds(oi * 64, 64), cols] = piece.astype(BF)

    def mixed_part(k):
        for n in (2 * k, 2 * k + 1):
            got(hid.at[half_rows(n, theirs)], d2r.at[0, n])

        @pl.loop(0, 7)
        def _(n):
            cols = pl.ds(pl.multiple_of(n * 256, 256), 256)
            put(0, k, cols, jnp.dot(
                hid[pl.ds(k * 512, 512), :], wdn[:, cols], preferred_element_type=F32
            ))

    def igrad_part(k):
        for n in (2 * k, 2 * k + 1):
            got(dgu.at[half_rows(n, theirs)], d2r.at[1, n])

        @pl.loop(0, 7)
        def _(n):
            cols = pl.ds(pl.multiple_of(n * 256, 256), 256)
            put(1, k, cols, lax.dot_general(
                dgu[pl.ds(k * 512, 512), :], wgu[cols, :], (((1,), (1,)), ((), ())),
                preferred_element_type=F32,
            ))

    def reduce_step(a, oi):
        i, j = IJ[oi]
        kids = [OI[i, kid] for kid, _ in KIDS[j]]
        if j == 0:
            kids += [OI[kid, 0] for kid, _ in KIDS[i]]
        if oi:
            if j:
                parent, axis = next(((i, p), 1) for p in KIDS for q, _ in KIDS[p] if q == j)
                way = next(w for p in KIDS for q, w in KIDS[p] if q == j)
            else:
                parent, axis = next(((p, 0), 0) for p in KIDS for q, _ in KIDS[p] if q == i)
                way = next(w for p in KIDS for q, w in KIDS[p] if q == i)

        @pl.loop(0, 4)
        def _(c):
            if kids:
                acc = keep[a, rows(KEPT.index((i, j)), c), :]
                for kid in kids:
                    got(rin.at[a, rows(kid, c)], rrecv.at[a, kid, c])
                    acc += rin[a, rows(kid, c), :].astype(F32)
                if oi:
                    par[a, rows(oi, c), :] = acc.astype(BF)
                else:
                    for h in range(2):
                        g = c * 2 + h
                        yse[a, g] = acc[h * 8 : h * 8 + 8]

                        @pl.when(g != f)
                        def _():
                            rc(yse.at[a, g], yor.at[a, f], fsend.at[a, g], frecv.at[a, f],
                               ring_dev(g)).start()
            if oi:
                rc(par.at[a, rows(oi, c)], rin.at[a, rows(oi, c)], rsend.at[a, oi, c],
                   rrecv.at[a, oi, c], xz_dev(c, axis, -way)).start()

    def finish(a):
        yor[a, f] = yse[a, f]

        @pl.loop(1, 8)
        def _(k):
            g = (f + k) % 8
            got(yor.at[a, g], frecv.at[a, g])

    def down_piece(n):
        cols = pl.ds(n * 256, 256)
        sdg[:, cols] = lax.dot_general(
            hid[...], big[1, :, cols], (((0,), (0,)), ((), ())), preferred_element_type=F32
        )

    def gate_up_piece(n):
        r = pl.ds(n * 256, 256)
        sgu[r, :] = lax.dot_general(
            big[0, :, r], dgu[...], (((0,), (0,)), ((), ())), preferred_element_type=F32
        )

    steps = {
        "T": functools.partial(gather_step, 0),
        "C": functools.partial(gather_step, 1),
        "GU": functools.partial(product, 0),
        "B": functools.partial(product, 1),
        "S": functools.partial(chip_sum, 0),
        "SB": functools.partial(chip_sum, 1),
        "R": functools.partial(relay_on, 0),
        "RB": functools.partial(relay_on, 1),
        "H": forward_act,
        "DB": backward_act,
        "M": mixed_part,
        "I": igrad_part,
        "RM": functools.partial(reduce_step, 0),
        "RI": functools.partial(reduce_step, 1),
        "WD": down_piece,
        "WG": gate_up_piece,
        "FM": finish,
        "FI": finish,
    }
    for word in PROGRAM:
        name = word.rstrip("0123456789")
        with jax.named_scope(word):
            steps[name](int(word[len(name):]))

    for a in range(2):
        @pl.loop(1, 8)
        def _(k):
            g = (f + k) % 8
            sent(yin.at[a, g], ysend.at[a, g])
            sent(yse.at[a, g], fsend.at[a, g])

        @pl.loop(4, 64)
        def _(n):
            oi, c = n // 4, n % 4
            sent(big.at[a, rows(oi, c)], gsend.at[a, oi, c])
            sent(par.at[a, rows(oi, c)], rsend.at[a, oi, c])
        for k in range(4):
            sent(part[a][1].at[k], d1s.at[a, k])
            for w in range(2):
                sent(part[a][3].at[k, w], e1s.at[a, k, w])
                sent(part[a][3].at[k, w], e2s.at[a, k, w])
            sent((hid, dgu)[a].at[half_rows(k, mine)], d2s.at[a, k])


PROGRAM = (
    "T0", "T1", "T3", "T2", "GU0", "T5", "S0", "T4", "T6", "T7", "GU1", "T10",
    "S1", "T9", "T11", "T14", "T8", "C0", "R0", "GU2", "S2", "T12", "R1", "T15",
    "T13", "GU3", "C1", "C3", "S3", "H0", "C2", "B0", "R2", "R3", "C5", "SB0",
    "H1", "H2", "C10", "C4", "C7", "C6", "B1", "M0", "H3", "RM4", "RB0", "SB1",
    "C11", "C9", "C8", "M1", "RM13", "RM12", "C13", "B2", "RM15", "C12", "RM10", "C14",
    "RM14", "SB2", "DB0", "C15", "B3", "RB1", "RM7", "SB3", "WD3", "RM9", "DB1", "RM11",
    "RM8", "RB2", "RM6", "RB3", "I0", "DB2", "RI4", "WD6", "DB3", "RM3", "RM2", "RM5",
    "I1", "RI15", "RI9", "RI12", "WD5", "WG1", "RI13", "WG6", "RI11", "WD0", "WD1", "RI14",
    "RI10", "WG5", "RI7", "RI6", "RI8", "RI5", "RM1", "WG2", "WD4", "RI3", "RI2", "WG3",
    "RI1", "WG0", "WD2", "WG4", "RM0", "RI0", "FM0", "FI1",
)


def write_out(sgu, sdg, yor, mixed, igrad, gg, ug, dg, sem):
    copies = (
        pltpu.make_async_copy(sgu.at[:, pl.ds(0, H)], gg, sem.at[0]),
        pltpu.make_async_copy(sgu.at[:, pl.ds(H, H)], ug, sem.at[1]),
        pltpu.make_async_copy(sdg, dg, sem.at[2]),
    )
    for cp in copies:
        cp.start()
    for a, out in ((0, mixed), (1, igrad)):
        for b in range(4):
            g = (b // 2) * 4 + b % 2
            out[:, pl.ds(b * DB, DB)] = (yor[a, g] + yor[a, g + 2]).astype(BF)
    for cp in copies:
        cp.wait()


def body(tokens, w_gate, w_up, w_down, cotangent):
    vmem = pl.BlockSpec(memory_space=pltpu.VMEM)
    anyw = pl.BlockSpec(memory_space=pl.ANY)
    dma = pltpu.SemaphoreType.DMA
    held = pl.pallas_call(
        kernel,
        name="ffn",
        out_shape=(
            pltpu.VMEM((DB, 2 * H), F32),
            pltpu.VMEM((H, DB), F32),
            pltpu.VMEM((2, 8, 8, DB), F32),
        ),
        in_specs=[anyw] * 5,
        out_specs=(vmem, vmem, vmem),
        scratch_shapes=[
            pltpu.VMEM((8, D), BF),
            pltpu.VMEM((8, D), BF),
            pltpu.VMEM((2, 8, 8, DB), BF),
            pltpu.VMEM((2, T, DB), BF),
            pltpu.VMEM((DB, 2 * H), BF),
            pltpu.VMEM((H, DB), BF),
            pltpu.VMEM((T, 2 * H), F32),
            pltpu.VMEM((4, HC, 2 * H), F32),
            pltpu.VMEM((4, HC, 2 * H), BF),
            pltpu.VMEM((4, 2, 64, 2 * H), BF),
            pltpu.VMEM((4, HC, 2 * H), BF),
            pltpu.VMEM((T, H), F32),
            pltpu.VMEM((4, HC, H), F32),
            pltpu.VMEM((4, HC, H), BF),
            pltpu.VMEM((4, 2, 64, H), BF),
            pltpu.VMEM((4, HC, H), BF),
            pltpu.VMEM((T // 2, H), F32),
            pltpu.VMEM((T // 2, H), F32),
            pltpu.VMEM((T, H), BF),
            pltpu.VMEM((T, 2 * H), BF),
            pltpu.VMEM((2, T, DB), BF),
            pltpu.VMEM((2, T // 2, DB), F32),
            pltpu.VMEM((2, T, DB), BF),
            pltpu.VMEM((2, 8, 8, DB), F32),
            dma((2, 8)), dma((2, 8)),
            dma((2, 16, 4)), dma((2, 16, 4)),
            dma((5,)),
            dma((2, 4)), dma((2, 4)),
            dma((2, 4, 2)), dma((2, 4, 2)),
            dma((2, 4, 2)), dma((2, 4, 2)),
            dma((2, 4)), dma((2, 4)),
            dma((2, 16, 4)), dma((2, 16, 4)),
            dma((2, 8)), dma((2, 8)),
        ],
        compiler_params=pltpu.CompilerParams(
            collective_id=0, has_side_effects=True, vmem_limit_bytes=52 * 1024 * 1024
        ),
    )(tokens, cotangent, w_gate, w_up, w_down)
    return pl.pallas_call(
        write_out,
        name="write_out",
        out_shape=(
            jax.ShapeDtypeStruct((8, D), BF),
            jax.ShapeDtypeStruct((8, D), BF),
            jax.ShapeDtypeStruct((DB, H), F32),
            jax.ShapeDtypeStruct((DB, H), F32),
            jax.ShapeDtypeStruct((H, DB), F32),
        ),
        in_specs=[vmem] * 3,
        out_specs=(vmem, vmem, anyw, anyw, anyw),
        scratch_shapes=[dma((3,))],
        compiler_params=pltpu.CompilerParams(vmem_limit_bytes=2 * 1024 * 1024),
    )(*held)


def solution(mesh):
    split = Mesh(mesh.devices.reshape(2, 2, 2, 4, 4), DP_TP)
    return jax.shard_map(
        body,
        mesh=split,
        in_specs=(P(DP_TP, None), P(None, TP), P(None, TP), P(TP, None), P(DP_TP, None)),
        out_specs=(P(DP_TP, None), P(DP_TP, None), P(DP, TP), P(DP, TP), P(TP, DP)),
        check_vma=False,
    )
```

```python
import functools

import jax
import jax.numpy as jnp
from jax import lax
from jax.experimental import pallas as pl
from jax.experimental.pallas import tpu as pltpu
from jax.sharding import Mesh
from jax.sharding import PartitionSpec as P

TP = ("yl", "x", "z")
DP = ("yh", "co")
DP_TP = DP + TP
BF = jnp.bfloat16
F32 = jnp.float32

D = 7168
DB = 1792
H = 384
T = 1024
CH = 256
HC = 128

KIDS = {0: ((1, 1), (3, -1)), 1: ((2, 1),), 2: (), 3: ()}
IJ = (
    (0, 0),
    (1, 0), (0, 1), (3, 0), (0, 3),
    (2, 0), (1, 1), (3, 1), (1, 3), (0, 2), (3, 3),
    (2, 1), (1, 2), (3, 2), (2, 3),
    (2, 2),
)
LEAVES = ((3, 3), (3, 2), (0, 3), (0, 2))
REDUCE_SHARED = (LEAVES[:2], LEAVES[:4])
KEPT = tuple(ij for ij in IJ if ij[1] < 2)
OI = {ij: n for n, ij in enumerate(IJ)}


def kernel(
    tok_in, cot_in, wg, wu, wd,
    sgu, sdg, yor,
    tok, cot, yin, big, wgu, wdn, gf, rb, xs, rl, yr, bf, rbb, xsb, rlb, yrb,
    sa, sd, hid, dgu, par, keep, rin, pex, yse,
    ysend, yrecv, gsend, grecv, wsem, d1s, d1r, e1s, e1r, e2s, e2r,
    d2s, d2r, rsend, rrecv, fsend, frecv, qsend, qrecv,
):
    yh, co, yl = lax.axis_index("yh"), lax.axis_index("co"), lax.axis_index("yl")
    x, z = lax.axis_index("x"), lax.axis_index("z")
    y = yh * 2 + yl
    f = y * 2 + co
    d = yh * 2 + co

    def ring_dev(g):
        gy = g // 2
        return {"yh": gy // 2, "yl": gy % 2, "co": g % 2}

    def y_dev(k):
        gy = (y + k) % 4
        return {"yh": gy // 2, "yl": gy % 2}

    def xz_dev(c, axis, way):
        s = (1 - 2 * (c % 2)) * way
        o = c // 2
        on_x = (1 - o) if axis == 0 else o
        return {"x": (x + s * on_x + 4) % 4, "z": (z + s * (1 - on_x) + 4) % 4}

    other = {"co": 1 - co}
    pair = {"yl": 1 - yl}

    def ours(n):
        return yl * (1 + n) + (1 - yl) * 3 * n

    def its(n):
        return (1 - yl) * (1 + n) + yl * 3 * n

    def rc(src, dst, ss, rs, dev):
        return pltpu.make_async_remote_copy(
            src_ref=src, dst_ref=dst, send_sem=ss, recv_sem=rs,
            device_id=dev, device_id_type=pl.DeviceIdType.MESH,
        )

    def got(dst, rs):
        rc(dst, dst, rs, rs, other).wait_recv()

    def sent(src, ss):
        rc(src, src, ss, ss, other).wait_send()

    w_copies = (
        pltpu.make_async_copy(wg.at[pl.ds(d * DB, DB), :], wgu.at[:, pl.ds(0, H)], wsem.at[0]),
        pltpu.make_async_copy(wu.at[pl.ds(d * DB, DB), :], wgu.at[:, pl.ds(H, H)], wsem.at[1]),
        pltpu.make_async_copy(wd.at[:, pl.ds(d * DB, DB)], wdn, wsem.at[2]),
    )
    in_copies = (
        pltpu.make_async_copy(tok_in, tok, wsem.at[3]),
        pltpu.make_async_copy(cot_in, cot, wsem.at[4]),
    )
    for cp in in_copies + w_copies:
        cp.start()

    barrier = pltpu.get_barrier_semaphore()
    for dev in ({"x": (x + 1) % 4}, {"x": (x + 3) % 4}, {"z": (z + 1) % 4}, {"z": (z + 3) % 4}):
        pl.semaphore_signal(barrier, inc=1, device_id=dev, device_id_type=pl.DeviceIdType.MESH)
    for k in range(1, 8):
        pl.semaphore_signal(
            barrier, inc=1, device_id=ring_dev((f + k) % 8), device_id_type=pl.DeviceIdType.MESH
        )
    pl.semaphore_wait(barrier, 11)

    for a, src in ((0, tok), (1, cot)):
        in_copies[a].wait()

        @pl.loop(0, 7)
        def _(n):
            k = (n + 1) // 2
            g = ((y + k + (k // 2) * (1 - 2 * (k // 3))) % 4) * 2 + (co + n + 1) % 2
            gd = (g // 4) * 2 + g % 2
            rc(
                src.at[:, pl.ds(pl.multiple_of(gd * DB, 128), DB)], yin.at[a, f],
                ysend.at[a], yrecv.at[a, f], ring_dev(g),
            ).start()
    for a, src in ((0, tok), (1, cot)):
        yin[a, f] = src[:, pl.ds(pl.multiple_of(d * DB, 128), DB)]

    def rows(oi, c):
        return pl.ds(pl.multiple_of(oi * 64 + c * 16, 16), 16)

    def near(n):
        return (y + n + (n // 2) * (1 - 2 * (n // 3))) % 4

    def along_second(a, oi, c):
        i, j = IJ[oi]
        src = big.at[a, rows(oi, c)]

        for kid, way in KIDS[j]:
            to = OI[i, kid]
            rc(src, big.at[a, rows(to, c)], gsend.at[a], grecv.at[a, to, c],
               xz_dev(c, 1, way)).start()

    def assemble(a, c):
        halves = []
        for h in range(2):
            g = c * 2 + h

            @pl.when(g != f)
            def _():
                got(yin.at[a, g], yrecv.at[a, g])

            halves.append(yin[a, g].astype(F32))
        big[a, rows(0, c), :] = jnp.concatenate(halves, axis=0).astype(BF)

    COLOURS = {"": (0, 4), "a": (0, 1), "b": (1, 4), "c": (1, 3), "d": (3, 4)}

    def gather_step(a, oi, which):
        i, j = IJ[oi]
        @pl.loop(*COLOURS[which])
        def _(n):
            c = near(n)
            if oi == 0:
                assemble(a, c)
            else:
                got(big.at[a, rows(oi, c)], grecv.at[a, oi, c])
            src = big.at[a, rows(oi, c)]
            if j == 0:
                for kid, way in KIDS[i]:
                    to = OI[kid, 0]
                    rc(src, big.at[a, rows(to, c)], gsend.at[a], grecv.at[a, to, c],
                       xz_dev(c, 0, way)).start()
            if oi:
                along_second(a, oi, c)

        if oi == 0:
            @pl.loop(*COLOURS[which])
            def _(n):
                along_second(a, oi, near(n))

    mine = HC * co
    theirs = HC - mine

    def half_rows(k, off):
        return pl.ds(pl.multiple_of(k * CH + off, HC), HC)

    part = ((gf, rb, xs, rl, yr), (bf, rbb, xsb, rlb, yrb))

    def product(a, k):
        full = part[a][0]
        left = big.at[a, pl.ds(k * CH, CH)]
        if a == 0:
            if k == 0:
                w_copies[0].wait()
                w_copies[1].wait()

            @pl.loop(0, 3)
            def _(n):
                cols = pl.ds(pl.multiple_of(n * 256, 256), 256)
                full[pl.ds(k * CH, CH), cols] = jnp.dot(
                    left[...], wgu[:, cols], preferred_element_type=F32
                )
        else:
            if k == 0:
                w_copies[2].wait()
            full[pl.ds(k * CH, CH), :] = lax.dot_general(
                left[...], wdn[...], (((1,), (1,)), ((), ())), preferred_element_type=F32
            )
        rc(full.at[half_rows(k, theirs)], part[a][1].at[k], d1s.at[a], d1r.at[a, k], other).start()

    def chip_sum(a, k):
        full, recv, out, relay, _ = part[a]
        got(recv.at[k], d1r.at[a, k])
        s = full[half_rows(k, mine), :] + recv[k]
        full[half_rows(k, mine), :] = s
        out[k] = s.astype(BF)
        for w, way in ((0, 1), (1, -1)):
            rc(out.at[k, pl.ds(w * 64, 64)], relay.at[k, w], e1s.at[a], e1r.at[a, k, w],
               y_dev(way + 4)).start()

    def relay_on(a, k):
        _, _, _, relay, recv = part[a]
        for w, way in ((0, 1), (1, -1)):
            got(relay.at[k, w], e1r.at[a, k, w])
            rc(relay.at[k, w], recv.at[k, pl.ds(w * 64, 64)], e2s.at[a], e2r.at[a, k, w],
               y_dev(way + 4)).start()

    def total(a, k, cols):
        full, _, _, _, recv = part[a]
        return full[half_rows(k, mine), cols] + recv[k, :, cols].astype(F32)

    def arrived(a, k):
        recv = part[a][4]
        for w in range(2):
            got(recv.at[k, pl.ds(w * 64, 64)], e2r.at[a, k, w])

    def forward_act(k):
        arrived(0, k)
        gate = total(0, k, pl.ds(0, H))
        up = total(0, k, pl.ds(H, H))
        sig = 1.0 / (1.0 + jnp.exp(-gate))
        act = gate * sig
        sa[pl.ds(k * HC, HC), :] = act
        sd[pl.ds(k * HC, HC), :] = up * sig * (1.0 + gate * (1.0 - sig))
        hid[half_rows(k, mine), :] = (act * up).astype(BF)
        rc(hid.at[half_rows(k, mine)], hid.at[half_rows(k, mine)], d2s.at[0], d2r.at[0, k], other).start()

    def backward_act(k):
        arrived(1, k)
        back = total(1, k, pl.ds(0, H))
        dgu[half_rows(k, mine), pl.ds(0, H)] = (back * sd[pl.ds(k * HC, HC), :]).astype(BF)
        dgu[half_rows(k, mine), pl.ds(H, H)] = (back * sa[pl.ds(k * HC, HC), :]).astype(BF)
        rc(dgu.at[half_rows(k, mine)], dgu.at[half_rows(k, mine)], d2s.at[1], d2r.at[1, k], other).start()

    def put(a, k, cols, r):
        for n in range(8):
            oi = 8 * k + n
            piece = r[n * 64 : n * 64 + 64]
            if IJ[oi] in KEPT:
                keep[a, pl.ds(KEPT.index(IJ[oi]) * 64, 64), cols] = piece
            else:
                par[a, pl.ds(oi * 64, 64), cols] = piece.astype(BF)

    def mixed_part(k):
        for n in (2 * k, 2 * k + 1):
            got(hid.at[half_rows(n, theirs)], d2r.at[0, n])

        for n in range(7):
            cols = pl.ds(n * 256, 256)
            put(0, k, cols, jnp.dot(
                hid[pl.ds(k * 512, 512), :], wdn[:, cols], preferred_element_type=F32
            ))

    def igrad_part(k):
        for n in (2 * k, 2 * k + 1):
            got(dgu.at[half_rows(n, theirs)], d2r.at[1, n])

        for n in range(7):
            cols = pl.ds(n * 256, 256)
            put(1, k, cols, lax.dot_general(
                dgu[pl.ds(k * 512, 512), :], wgu[cols, :], (((1,), (1,)), ((), ())),
                preferred_element_type=F32,
            ))

    def reduce_step(a, oi, which):
        i, j = IJ[oi]
        kids = [OI[i, kid] for kid, _ in KIDS[j] if (i, kid) not in REDUCE_SHARED[a]]
        if j == 0:
            kids += [OI[kid, 0] for kid, _ in KIDS[i]]
        if oi:
            along = j or i
            parent, way = next((p, w) for p in KIDS for q, w in KIDS[p] if q == along)
            above, axis = ((i, parent), 1) if j else ((parent, 0), 0)

        def send(c):
            rc(par.at[a, rows(oi, c)], rin.at[a, rows(oi, c)], rsend.at[a],
               rrecv.at[a, oi, c], xz_dev(c, axis, -way)).start()

        if which:
            leaf = LEAVES.index((i, j)) if (i, j) in LEAVES else None
        if which == "y":
            @pl.loop(0, 2)
            def _(n):
                rc(par.at[a, rows(oi, its(n))], pex.at[a, leaf, n], qsend.at[a],
                   qrecv.at[a, leaf, n], pair).start()
            return
        if which == "x":
            @pl.loop(0, 2)
            def _(n):
                c = ours(n)
                got(pex.at[a, leaf, n], qrecv.at[a, leaf, n])
                par[a, rows(oi, c), :] = (
                    par[a, rows(oi, c), :].astype(F32) + pex[a, leaf, n].astype(F32)
                ).astype(BF)
                send(c)
            return
        if which == "k":
            @pl.loop(0, 2)
            def _(n):
                c = ours(n)
                got(rin.at[a, rows(oi, c)], rrecv.at[a, oi, c])
                keep[a, rows(KEPT.index(above), c), :] += rin[a, rows(oi, c), :].astype(F32)
            return

        @pl.loop(*COLOURS[which])
        def _(n):
            c = near(3 - n) if which == "" else near(n)
            if (i, j) in KEPT:
                acc = keep[a, rows(KEPT.index((i, j)), c), :]
                for kid in kids:
                    got(rin.at[a, rows(kid, c)], rrecv.at[a, kid, c])
                    acc += rin[a, rows(kid, c), :].astype(F32)
                if oi:
                    par[a, rows(oi, c), :] = acc.astype(BF)
                else:
                    for h in range(2):
                        g = c * 2 + h
                        yse[a, g] = acc[h * 8 : h * 8 + 8]

                        @pl.when(g != f)
                        def _():
                            rc(yse.at[a, g], yor.at[a, f], fsend.at[a], frecv.at[a, f],
                               ring_dev(g)).start()
            if oi:
                send(c)

    def finish(a):
        yor[a, f] = yse[a, f]

        @pl.loop(1, 8)
        def _(k):
            g = (f + k) % 8
            got(yor.at[a, g], frecv.at[a, g])

    def down_piece(n):
        cols = pl.ds(n * 256, 256)
        sdg[:, cols] = lax.dot_general(
            hid[...], big[1, :, cols], (((0,), (0,)), ((), ())), preferred_element_type=F32
        )

    def gate_up_piece(n):
        r = pl.ds(n * 256, 256)
        sgu[r, :] = lax.dot_general(
            big[0, :, r], dgu[...], (((0,), (0,)), ((), ())), preferred_element_type=F32
        )

    steps = {
        "T": functools.partial(gather_step, 0),
        "C": functools.partial(gather_step, 1),
        "GU": functools.partial(product, 0),
        "B": functools.partial(product, 1),
        "S": functools.partial(chip_sum, 0),
        "SB": functools.partial(chip_sum, 1),
        "R": functools.partial(relay_on, 0),
        "RB": functools.partial(relay_on, 1),
        "H": forward_act,
        "DB": backward_act,
        "M": mixed_part,
        "I": igrad_part,
        "RM": functools.partial(reduce_step, 0),
        "RI": functools.partial(reduce_step, 1),
        "WD": down_piece,
        "WG": gate_up_piece,
        "FM": finish,
        "FI": finish,
    }
    for word in PROGRAM:
        name = word.rstrip("abcdkxy").rstrip("0123456789")
        number = word[len(name):].rstrip("abcdkxy")
        which = word[len(name) + len(number):]
        with jax.named_scope(word):
            if name in ("T", "C", "RM", "RI"):
                steps[name](int(number), which)
            else:
                steps[name](int(number))

    for a in range(2):
        sent(yin.at[a, pl.ds(0, 7)], ysend.at[a])
        sent(big.at[a, pl.ds(0, 15 * 64)], gsend.at[a])
        sent(part[a][1], d1s.at[a])
        sent(part[a][3], e1s.at[a])
        sent(part[a][3], e2s.at[a])
        sent((hid, dgu)[a].at[pl.ds(0, T // 2)], d2s.at[a])
        shared = len(REDUCE_SHARED[a])
        sent(pex.at[a, pl.ds(0, shared)], qsend.at[a])
        sent(par.at[a, pl.ds(0, 15 * 64 - 32 * shared)], rsend.at[a])
        sent(yse.at[a, pl.ds(0, 7)], fsend.at[a])


PROGRAM = (
    "T0a", "T0c", "T4a", "T0d", "T1a", "T2a", "T3a", "T1b", "T3b", "T2b", "GU0", "T5",
    "T6", "S0", "T4b", "T7", "GU1", "T10", "S1", "T9", "T8", "T11", "GU2", "T14",
    "C0", "R0", "T12", "S2", "T13", "R1", "T15", "GU3", "H0", "C3", "S3", "C1",
    "C2", "R2", "H1", "B0", "R3", "M0", "RM4", "SB0", "C5", "C7", "C4", "C6",
    "B1", "H2", "H3", "C9", "SB1", "RB0", "C10", "M1", "RM10y", "C11", "RM15", "RM13y",
    "RM12", "C14", "RM9", "C13", "RM14", "RB1", "C12", "C8", "DB0", "B2", "C15", "B3",
    "SB2", "RM11", "SB3", "RM6", "DB1", "RM13x", "RB2", "RM8", "WD0", "RB3", "RM5", "RM10x",
    "I0", "DB2", "RM2", "DB3", "RM13k", "RM7", "RI4y", "RM1", "I1", "RI15", "RI13y", "WD4",
    "RI9y", "RI12", "RM10k", "RM3", "RI14", "RI10y", "WG3", "WD5", "RI11", "RI6", "WD2", "RI13x",
    "RI8", "RM0", "RI4x", "RI9x", "WG5", "RI5b", "WD1", "RI10x", "WG4", "RI13k", "RI7", "WD3",
    "RI4k", "RI5a", "WD6", "RI9k", "RI2b", "RI2a", "RI1b", "RI10k", "RI3b", "WG2", "RI1a", "RI0d",
    "WG1", "RI0c", "FM0", "RI3a", "WG0", "RI0a", "WG6", "FI1",
)


def write_out(sgu, sdg, yor, mixed, igrad, gg, ug, dg, rows, sem):
    copies = [
        pltpu.make_async_copy(sgu.at[:, pl.ds(0, H)], gg, sem.at[0]),
        pltpu.make_async_copy(sgu.at[:, pl.ds(H, H)], ug, sem.at[1]),
        pltpu.make_async_copy(sdg, dg, sem.at[2]),
    ]
    for cp in copies:
        cp.start()
    for a, out in ((0, mixed), (1, igrad)):
        for b in range(4):
            g = (b // 2) * 4 + b % 2
            rows[a, :, pl.ds(b * DB, DB)] = (yor[a, g] + yor[a, g + 2]).astype(BF)
        copies.append(pltpu.make_async_copy(rows.at[a], out, sem.at[3 + a]))
        copies[-1].start()
    for cp in copies:
        cp.wait()


def body(tokens, w_gate, w_up, w_down, cotangent):
    vmem = pl.BlockSpec(memory_space=pltpu.VMEM)
    anyw = pl.BlockSpec(memory_space=pl.ANY)
    dma = pltpu.SemaphoreType.DMA
    held = pl.pallas_call(
        kernel,
        name="ffn",
        out_shape=(
            pltpu.VMEM((DB, 2 * H), F32),
            pltpu.VMEM((H, DB), F32),
            pltpu.VMEM((2, 8, 8, DB), F32),
        ),
        in_specs=[anyw] * 5,
        out_specs=(vmem, vmem, vmem),
        scratch_shapes=[
            pltpu.VMEM((8, D), BF),
            pltpu.VMEM((8, D), BF),
            pltpu.VMEM((2, 8, 8, DB), BF),
            pltpu.VMEM((2, T, DB), BF),
            pltpu.VMEM((DB, 2 * H), BF),
            pltpu.VMEM((H, DB), BF),
            pltpu.VMEM((T, 2 * H), F32),
            pltpu.VMEM((4, HC, 2 * H), F32),
            pltpu.VMEM((4, HC, 2 * H), BF),
            pltpu.VMEM((4, 2, 64, 2 * H), BF),
            pltpu.VMEM((4, HC, 2 * H), BF),
            pltpu.VMEM((T, H), F32),
            pltpu.VMEM((4, HC, H), F32),
            pltpu.VMEM((4, HC, H), BF),
            pltpu.VMEM((4, 2, 64, H), BF),
            pltpu.VMEM((4, HC, H), BF),
            pltpu.VMEM((T // 2, H), F32),
            pltpu.VMEM((T // 2, H), F32),
            pltpu.VMEM((T, H), BF),
            pltpu.VMEM((T, 2 * H), BF),
            pltpu.VMEM((2, T, DB), BF),
            pltpu.VMEM((2, T // 2, DB), F32),
            pltpu.VMEM((2, T, DB), BF),
            pltpu.VMEM((2, 4, 2, 16, DB), BF),
            pltpu.VMEM((2, 8, 8, DB), F32),
            dma((2,)), dma((2, 8)),
            dma((2,)), dma((2, 16, 4)),
            dma((5,)),
            dma((2,)), dma((2, 4)),
            dma((2,)), dma((2, 4, 2)),
            dma((2,)), dma((2, 4, 2)),
            dma((2,)), dma((2, 4)),
            dma((2,)), dma((2, 16, 4)),
            dma((2,)), dma((2, 8)),
            dma((2,)), dma((2, 4, 2)),
        ],
        compiler_params=pltpu.CompilerParams(
            collective_id=0, has_side_effects=True, vmem_limit_bytes=53 * 1024 * 1024
        ),
    )(tokens, cotangent, w_gate, w_up, w_down)
    return pl.pallas_call(
        write_out,
        name="write_out",
        out_shape=(
            jax.ShapeDtypeStruct((8, D), BF),
            jax.ShapeDtypeStruct((8, D), BF),
            jax.ShapeDtypeStruct((DB, H), F32),
            jax.ShapeDtypeStruct((DB, H), F32),
            jax.ShapeDtypeStruct((H, DB), F32),
        ),
        in_specs=[vmem] * 3,
        out_specs=(anyw,) * 5,
        scratch_shapes=[pltpu.VMEM((2, 8, D), BF), dma((5,))],
        compiler_params=pltpu.CompilerParams(vmem_limit_bytes=2 * 1024 * 1024),
    )(*held)


def solution(mesh):
    split = Mesh(mesh.devices.reshape(2, 2, 2, 4, 4), DP_TP)
    return jax.shard_map(
        body,
        mesh=split,
        in_specs=(P(DP_TP, None), P(None, TP), P(None, TP), P(TP, None), P(DP_TP, None)),
        out_specs=(P(DP_TP, None), P(DP_TP, None), P(DP, TP), P(DP, TP), P(TP, DP)),
        check_vma=False,
    )
```

```python
import functools

import jax
import jax.numpy as jnp
from jax import lax
from jax.experimental import pallas as pl
from jax.experimental.pallas import tpu as pltpu
from jax.sharding import Mesh
from jax.sharding import PartitionSpec as P

TP = ("yl", "x", "z")
DP = ("yh", "co")
DP_TP = DP + TP
BF = jnp.bfloat16
F32 = jnp.float32

D = 7168
DB = 1792
H = 384
T = 1024
CH = 256
HC = 128

KIDS = {0: ((1, 1), (3, -1)), 1: ((2, 1),), 2: (), 3: ()}
IJ = (
    (0, 0),
    (1, 0), (0, 1), (3, 0), (0, 3),
    (2, 0), (1, 1), (3, 1), (1, 3), (0, 2), (3, 3),
    (2, 1), (1, 2), (3, 2), (2, 3),
    (2, 2),
)
LEAVES = ((3, 3), (3, 2), (0, 3), (0, 2))
REDUCE_SHARED = (LEAVES[:2], LEAVES[:2])
KEPT = tuple(ij for ij in IJ if ij[1] < 2)
OI = {ij: n for n, ij in enumerate(IJ)}


def kernel(
    tok_in, cot_in, wg, wu, wd,
    sgu, sdg, yor,
    tok, cot, yin, big, wgu, wdn, gf, rb, xs, rl, yr, bf, rbb, xsb, rlb, yrb,
    sa, sd, hid, dgu, par, keep, rin, pex, yse, far_out, far_in,
    ysend, yrecv, gsend, grecv, wsem, d1s, d1r, e1s, e1r, e2s, e2r,
    d2s, d2r, rsend, rrecv, fsend, frecv, qsend, qrecv,
):
    yh, co, yl = lax.axis_index("yh"), lax.axis_index("co"), lax.axis_index("yl")
    x, z = lax.axis_index("x"), lax.axis_index("z")
    y = yh * 2 + yl
    f = y * 2 + co
    d = yh * 2 + co

    def ring_dev(g):
        gy = g // 2
        return {"yh": gy // 2, "yl": gy % 2, "co": g % 2}

    def y_dev(k):
        gy = (y + k) % 4
        return {"yh": gy // 2, "yl": gy % 2}

    def xz_dev(c, axis, way):
        s = (1 - 2 * (c % 2)) * way
        o = c // 2
        on_x = (1 - o) if axis == 0 else o
        return {"x": (x + s * on_x + 4) % 4, "z": (z + s * (1 - on_x) + 4) % 4}

    other = {"co": 1 - co}
    pair = {"yl": 1 - yl}

    def ours(n):
        return yl * (1 + n) + (1 - yl) * 3 * n

    def its(n):
        return (1 - yl) * (1 + n) + yl * 3 * n

    def rc(src, dst, ss, rs, dev):
        return pltpu.make_async_remote_copy(
            src_ref=src, dst_ref=dst, send_sem=ss, recv_sem=rs,
            device_id=dev, device_id_type=pl.DeviceIdType.MESH,
        )

    def got(dst, rs):
        rc(dst, dst, rs, rs, other).wait_recv()

    def sent(src, ss):
        rc(src, src, ss, ss, other).wait_send()

    w_copies = (
        pltpu.make_async_copy(wg.at[pl.ds(d * DB, DB), :], wgu.at[:, pl.ds(0, H)], wsem.at[0]),
        pltpu.make_async_copy(wu.at[pl.ds(d * DB, DB), :], wgu.at[:, pl.ds(H, H)], wsem.at[1]),
        pltpu.make_async_copy(wd.at[:, pl.ds(d * DB, DB)], wdn, wsem.at[2]),
    )
    in_copies = (
        pltpu.make_async_copy(tok_in, tok, wsem.at[3]),
        pltpu.make_async_copy(cot_in, cot, wsem.at[4]),
    )
    for cp in in_copies + w_copies:
        cp.start()

    barrier = pltpu.get_barrier_semaphore()
    for dev in ({"x": (x + 1) % 4}, {"x": (x + 3) % 4}, {"z": (z + 1) % 4}, {"z": (z + 3) % 4}):
        pl.semaphore_signal(barrier, inc=1, device_id=dev, device_id_type=pl.DeviceIdType.MESH)
    for k in range(1, 8):
        pl.semaphore_signal(
            barrier, inc=1, device_id=ring_dev((f + k) % 8), device_id_type=pl.DeviceIdType.MESH
        )
    pl.semaphore_wait(barrier, 11)

    for a, src in ((0, tok), (1, cot)):
        in_copies[a].wait()

        @pl.loop(0, 7)
        def _(n):
            k = (n + 1) // 2
            g = ((y + k + (k // 2) * (1 - 2 * (k // 3))) % 4) * 2 + (co + n + 1) % 2
            gd = (g // 4) * 2 + g % 2
            rc(
                src.at[:, pl.ds(pl.multiple_of(gd * DB, 128), DB)], yin.at[a, f],
                ysend.at[a], yrecv.at[a, (k + 1) // 2], ring_dev(g),
            ).start()
    for a, src in ((0, tok), (1, cot)):
        yin[a, f] = src[:, pl.ds(pl.multiple_of(d * DB, 128), DB)]

    def rows(oi, c):
        return pl.ds(pl.multiple_of(oi * 64 + c * 16, 16), 16)

    def sem_of(table, a, oi, c):
        base, n = table[a, oi]
        r = (c - y + 4) % 4
        return base + (0 if n == 1 else (r + 3) // 4 if n == 2 else r - (r // 3) * 2)

    def got_blocks(table, sems, buf, a, oi, which):
        part = "acd".find(which) if which in "acd" and which else 1 if which else 0
        lo, hi = COLOURS[which]
        got(buf.at[a, pl.ds(oi * 64, 16 * (hi - lo))], sems.at[table[a, oi][0] + part])

    def near(n):
        return (y + n + (n // 2) * (1 - 2 * (n // 3))) % 4

    def along_second(a, oi, c):
        i, j = IJ[oi]
        src = big.at[a, rows(oi, c)]

        for kid, way in KIDS[j]:
            to = OI[i, kid]
            rc(src, big.at[a, rows(to, c)], gsend.at[a], grecv.at[sem_of(GATHER_SEM, a, to, c)],
               xz_dev(c, 1, way)).start()

    def assemble(a, c):
        halves = [yin[a, c * 2 + h].astype(F32) for h in range(2)]
        big[a, rows(0, c), :] = jnp.concatenate(halves, axis=0).astype(BF)

    def gather_step(a, oi, which):
        i, j = IJ[oi]
        if oi:
            got_blocks(GATHER_SEM, grecv, big, a, oi, which)
        else:
            for part, (w, count) in enumerate((("a", 1), ("bc", 4), ("bd", 2))):
                if which in w or not which:
                    got(yin.at[a, pl.ds(0, count)], yrecv.at[a, part])

        @pl.loop(*COLOURS[which])
        def _(n):
            c = near(n)
            if oi == 0:
                assemble(a, c)
            src = big.at[a, rows(oi, c)]
            if j == 0:
                for kid, way in KIDS[i]:
                    to = OI[kid, 0]
                    rc(src, big.at[a, rows(to, c)], gsend.at[a], grecv.at[sem_of(GATHER_SEM, a, to, c)],
                       xz_dev(c, 0, way)).start()
            if oi:
                along_second(a, oi, c)

        if oi == 0:
            @pl.loop(*COLOURS[which])
            def _(n):
                along_second(a, oi, near(n))

    mine = HC * co
    theirs = HC - mine

    def half_rows(k, off):
        return pl.ds(pl.multiple_of(k * CH + off, HC), HC)

    part = ((gf, rb, xs, rl, yr), (bf, rbb, xsb, rlb, yrb))

    def product(a, k):
        full = part[a][0]
        left = big.at[a, pl.ds(k * CH, CH)]
        if a == 0:
            if k == 0:
                w_copies[0].wait()
                w_copies[1].wait()

            @pl.loop(0, 3)
            def _(n):
                cols = pl.ds(pl.multiple_of(n * 256, 256), 256)
                full[pl.ds(k * CH, CH), cols] = jnp.dot(
                    left[...], wgu[:, cols], preferred_element_type=F32
                )
        else:
            if k == 0:
                w_copies[2].wait()
            full[pl.ds(k * CH, CH), :] = lax.dot_general(
                left[...], wdn[...], (((1,), (1,)), ((), ())), preferred_element_type=F32
            )
        rc(full.at[half_rows(k, theirs)], part[a][1].at[k], d1s.at[a], d1r.at[a, k], other).start()

    def chip_sum(a, k):
        full, recv, out, relay, _ = part[a]
        got(recv.at[k], d1r.at[a, k])
        s = full[half_rows(k, mine), :] + recv[k]
        full[half_rows(k, mine), :] = s
        out[k] = s.astype(BF)
        for w, way in ((0, 1), (1, -1)):
            rc(out.at[k, pl.ds(w * 64, 64)], relay.at[k, w], e1s.at[a], e1r.at[a, k],
               y_dev(way + 4)).start()

    def relay_on(a, k):
        _, _, _, relay, recv = part[a]
        got(relay.at[k], e1r.at[a, k])
        for w, way in ((0, 1), (1, -1)):
            rc(relay.at[k, w], recv.at[k, pl.ds(w * 64, 64)], e2s.at[a], e2r.at[a, k],
               y_dev(way + 4)).start()

    def total(a, k, cols):
        full, _, _, _, recv = part[a]
        return full[half_rows(k, mine), cols] + recv[k, :, cols].astype(F32)

    def arrived(a, k):
        got(part[a][4].at[k], e2r.at[a, k])

    def forward_act(k):
        arrived(0, k)
        gate = total(0, k, pl.ds(0, H))
        up = total(0, k, pl.ds(H, H))
        sig = 1.0 / (1.0 + jnp.exp(-gate))
        act = gate * sig
        sa[pl.ds(k * HC, HC), :] = act
        sd[pl.ds(k * HC, HC), :] = up * sig * (1.0 + gate * (1.0 - sig))
        hid[half_rows(k, mine), :] = (act * up).astype(BF)
        rc(hid.at[half_rows(k, mine)], hid.at[half_rows(k, mine)], d2s.at[0], d2r.at[0, k], other).start()

    def backward_act(k):
        arrived(1, k)
        back = total(1, k, pl.ds(0, H))
        dgu[half_rows(k, mine), pl.ds(0, H)] = (back * sd[pl.ds(k * HC, HC), :]).astype(BF)
        dgu[half_rows(k, mine), pl.ds(H, H)] = (back * sa[pl.ds(k * HC, HC), :]).astype(BF)
        rc(dgu.at[half_rows(k, mine)], dgu.at[half_rows(k, mine)], d2s.at[1], d2r.at[1, k], other).start()

    def put(a, k, cols, r):
        for n in range(8):
            oi = 8 * k + n
            piece = r[n * 64 : n * 64 + 64]
            if IJ[oi] in KEPT:
                keep[a, pl.ds(KEPT.index(IJ[oi]) * 64, 64), cols] = piece
            else:
                par[a, pl.ds(oi * 64, 64), cols] = piece.astype(BF)

    def mixed_part(k):
        for n in (2 * k, 2 * k + 1):
            got(hid.at[half_rows(n, theirs)], d2r.at[0, n])

        for n in range(7):
            cols = pl.ds(n * 256, 256)
            put(0, k, cols, jnp.dot(
                hid[pl.ds(k * 512, 512), :], wdn[:, cols], preferred_element_type=F32
            ))

    def igrad_part(k):
        for n in (2 * k, 2 * k + 1):
            got(dgu.at[half_rows(n, theirs)], d2r.at[1, n])

        for n in range(7):
            cols = pl.ds(n * 256, 256)
            put(1, k, cols, lax.dot_general(
                dgu[pl.ds(k * 512, 512), :], wgu[cols, :], (((1,), (1,)), ((), ())),
                preferred_element_type=F32,
            ))

    def reduce_step(a, oi, which):
        i, j = IJ[oi]
        kids = [OI[i, kid] for kid, _ in KIDS[j] if (i, kid) not in REDUCE_SHARED[a]]
        if j == 0:
            kids += [OI[kid, 0] for kid, _ in KIDS[i]]
        if oi:
            way = next(w for p in KIDS for q, w in KIDS[p] if q == (j or i))
            axis = 1 if j else 0

        def send(c):
            rc(par.at[a, rows(oi, c)], rin.at[a, rows(oi, c)], rsend.at[a],
               rrecv.at[sem_of(REDUCE_SEM, a, oi, c)], xz_dev(c, axis, -way)).start()

        if which:
            leaf = LEAVES.index((i, j)) if (i, j) in LEAVES else None
        if which == "y":
            @pl.loop(0, 2)
            def _(n):
                rc(par.at[a, rows(oi, its(n))], pex.at[a, leaf, n], qsend.at[a],
                   qrecv.at[a, leaf], pair).start()
            return
        if which == "x":
            got(pex.at[a, leaf], qrecv.at[a, leaf])

            @pl.loop(0, 2)
            def _(n):
                c = ours(n)
                par[a, rows(oi, c), :] = (
                    par[a, rows(oi, c), :].astype(F32) + pex[a, leaf, n].astype(F32)
                ).astype(BF)
                send(c)
            return
        if which == "k":
            got(rin.at[a, pl.ds(oi * 64, 32)], rrecv.at[REDUCE_SEM[a, oi][0]])

            @pl.loop(0, 2)
            def _(n):
                c = ours(n)
                keep[a, rows(KEPT.index(above(oi)), c), :] += rin[a, rows(oi, c), :].astype(F32)
            return

        for kid in kids:
            got_blocks(REDUCE_SEM, rrecv, rin, a, kid, which)

        @pl.loop(*COLOURS[which])
        def _(n):
            c = near(3 - n) if which == "" else near(n)
            if (i, j) in KEPT:
                acc = keep[a, rows(KEPT.index((i, j)), c), :]
                for kid in kids:
                    acc += rin[a, rows(kid, c), :].astype(F32)
                if oi:
                    par[a, rows(oi, c), :] = acc.astype(BF)
                else:
                    for h in range(2):
                        g = c * 2 + h
                        piece = acc[h * 8 : h * 8 + 8]
                        far = c == (y + 2) % 4

                        @pl.when(far)
                        def _():
                            far_out[a, h] = piece.astype(BF)
                            rc(far_out.at[a, h], far_in.at[a, co], fsend.at[a, 1], frecv.at[a, 1],
                               ring_dev(g)).start()

                        @pl.when(jnp.logical_not(far))
                        def _():
                            yse[a, g] = piece

                        @pl.when(jnp.logical_not(far | (g == f)))
                        def _():
                            rc(yse.at[a, g], yor.at[a, f], fsend.at[a, 0], frecv.at[a, 0],
                               ring_dev(g)).start()
            if oi:
                send(c)

    def finish(a):
        yor[a, f] = yse[a, f]
        got(yor.at[a, pl.ds(0, 5)], frecv.at[a, 0])
        got(far_in.at[a], frecv.at[a, 1])
        for h in range(2):
            yor[a, ((y + 2) % 4) * 2 + h] = far_in[a, h].astype(F32)

    def down_piece(n):
        cols = pl.ds(n * 1024, 1024 - 256 * n)
        sdg[:, cols] = lax.dot_general(
            hid[...], big[1, :, cols], (((0,), (0,)), ((), ())), preferred_element_type=F32
        )

    def gate_up_piece(n):
        r = pl.ds(n * 256, 256)
        sgu[r, :] = lax.dot_general(
            big[0, :, r], dgu[...], (((0,), (0,)), ((), ())), preferred_element_type=F32
        )

    steps = {
        "T": functools.partial(gather_step, 0),
        "C": functools.partial(gather_step, 1),
        "GU": functools.partial(product, 0),
        "B": functools.partial(product, 1),
        "S": functools.partial(chip_sum, 0),
        "SB": functools.partial(chip_sum, 1),
        "R": functools.partial(relay_on, 0),
        "RB": functools.partial(relay_on, 1),
        "H": forward_act,
        "DB": backward_act,
        "M": mixed_part,
        "I": igrad_part,
        "RM": functools.partial(reduce_step, 0),
        "RI": functools.partial(reduce_step, 1),
        "WD": down_piece,
        "WG": gate_up_piece,
        "FM": finish,
        "FI": finish,
    }
    for word in PROGRAM:
        name, number, which = split_word(word)
        with jax.named_scope(word):
            if name in ("T", "C", "RM", "RI"):
                steps[name](number, which)
            else:
                steps[name](number)

    for a in range(2):
        sent(yin.at[a, pl.ds(0, 7)], ysend.at[a])
        sent(big.at[a, pl.ds(0, 15 * 64)], gsend.at[a])
        sent(part[a][1], d1s.at[a])
        sent(part[a][3], e1s.at[a])
        sent(part[a][3], e2s.at[a])
        sent((hid, dgu)[a].at[pl.ds(0, T // 2)], d2s.at[a])
        shared = len(REDUCE_SHARED[a])
        sent(pex.at[a, pl.ds(0, shared)], qsend.at[a])
        sent(par.at[a, pl.ds(0, 15 * 64 - 32 * shared)], rsend.at[a])
        sent(yse.at[a, pl.ds(0, 5)], fsend.at[a, 0])
        sent(far_out.at[a], fsend.at[a, 1])


PROGRAM = (
    "T0a", "C0a", "T1a", "T0c", "T0d", "C0b", "T1b", "T3a", "T4b", "T3b", "T4a", "T2b",
    "T2a", "GU0", "S0", "T5", "T6", "T7", "GU1", "T8", "T10", "T9", "R0", "S1",
    "T11", "GU2", "C1", "T14", "T13", "C3", "T12", "C2", "S2", "T15", "GU3", "R1",
    "S3", "C5", "H0", "R2", "C6", "C4", "B0", "H1", "C7", "R3", "M0", "C11",
    "C8", "C9", "C10", "B1", "RM4", "H2", "B2", "C13", "C12", "SB1", "C14", "H3",
    "SB2", "C15", "B3", "SB0", "M1", "RM15", "SB3", "RM12", "RM9", "RB1", "RM14", "WD1",
    "RB2", "RB3", "RB0", "RM11", "RM6", "RM8", "RM10y", "DB2", "DB3", "RM13y", "RM2", "RM5",
    "I1", "RI15", "RI8", "RI13y", "RM10x", "DB1", "RI10y", "RI12", "DB0", "RM13x", "RM1", "RI11",
    "I0", "WG4", "RI14", "WG1", "RI13x", "RM13k", "RM7", "RI10x", "RI6", "WG6", "WD0", "RI5",
    "RI13k", "RI7", "RM10k", "WG0", "RM3", "WG5", "RI10k", "RI9", "WG3", "RI4", "WG2", "RI3a",
    "RI3b", "RI1b", "RM0", "RI2b", "RI0d", "RI2a", "RI1a", "RI0c", "RI0a", "FM0", "FI1",
)


COLOURS = {"": (0, 4), "a": (0, 1), "b": (1, 4), "c": (1, 3), "d": (3, 4)}


def split_word(word):
    name = word.rstrip("abcdkxy").rstrip("0123456789")
    number = word[len(name):].rstrip("abcdkxy")
    return name, int(number), word[len(name) + len(number):]


def parts_of(name, oi):
    which = {w for a, n, w in map(split_word, PROGRAM) if a == name and n == oi}
    return 3 if "d" in which else 2 if "a" in which else 1


def above(oi):
    i, j = IJ[oi]
    up = next(p for p in KIDS for q, _ in KIDS[p] if q == (j or i))
    return (i, up) if j else (up, 0)


def tables():
    gather, reduce, at = {}, {}, [0, 0]
    for a in range(2):
        for oi in range(1, 16):
            n = parts_of("TC"[a], oi)
            gather[a, oi] = at[0], n
            at[0] += n
            n = 1 if IJ[oi] in REDUCE_SHARED[a] else parts_of(("RM", "RI")[a], OI[above(oi)])
            reduce[a, oi] = at[1], n
            at[1] += n
    return gather, reduce, at


GATHER_SEM, REDUCE_SEM, SEMS = tables()


def write_out(sgu, sdg, yor, mixed, igrad, gg, ug, dg, rows, sem):
    copies = [
        pltpu.make_async_copy(sgu.at[:, pl.ds(0, H)], gg, sem.at[0]),
        pltpu.make_async_copy(sgu.at[:, pl.ds(H, H)], ug, sem.at[1]),
        pltpu.make_async_copy(sdg, dg, sem.at[2]),
    ]
    for cp in copies:
        cp.start()
    for a, out in ((0, mixed), (1, igrad)):
        for b in range(4):
            g = (b // 2) * 4 + b % 2
            rows[a, :, pl.ds(b * DB, DB)] = (yor[a, g] + yor[a, g + 2]).astype(BF)
        copies.append(pltpu.make_async_copy(rows.at[a], out, sem.at[3 + a]))
        copies[-1].start()
    for cp in copies:
        cp.wait()


def body(tokens, w_gate, w_up, w_down, cotangent):
    vmem = pl.BlockSpec(memory_space=pltpu.VMEM)
    anyw = pl.BlockSpec(memory_space=pl.ANY)
    dma = pltpu.SemaphoreType.DMA
    held = pl.pallas_call(
        kernel,
        name="ffn",
        out_shape=(
            pltpu.VMEM((DB, 2 * H), F32),
            pltpu.VMEM((H, DB), F32),
            pltpu.VMEM((2, 8, 8, DB), F32),
        ),
        in_specs=[anyw] * 5,
        out_specs=(vmem, vmem, vmem),
        scratch_shapes=[
            pltpu.VMEM((8, D), BF),
            pltpu.VMEM((8, D), BF),
            pltpu.VMEM((2, 8, 8, DB), BF),
            pltpu.VMEM((2, T, DB), BF),
            pltpu.VMEM((DB, 2 * H), BF),
            pltpu.VMEM((H, DB), BF),
            pltpu.VMEM((T, 2 * H), F32),
            pltpu.VMEM((4, HC, 2 * H), F32),
            pltpu.VMEM((4, HC, 2 * H), BF),
            pltpu.VMEM((4, 2, 64, 2 * H), BF),
            pltpu.VMEM((4, HC, 2 * H), BF),
            pltpu.VMEM((T, H), F32),
            pltpu.VMEM((4, HC, H), F32),
            pltpu.VMEM((4, HC, H), BF),
            pltpu.VMEM((4, 2, 64, H), BF),
            pltpu.VMEM((4, HC, H), BF),
            pltpu.VMEM((T // 2, H), F32),
            pltpu.VMEM((T // 2, H), F32),
            pltpu.VMEM((T, H), BF),
            pltpu.VMEM((T, 2 * H), BF),
            pltpu.VMEM((2, T, DB), BF),
            pltpu.VMEM((2, T // 2, DB), F32),
            pltpu.VMEM((2, T, DB), BF),
            pltpu.VMEM((2, 4, 2, 16, DB), BF),
            pltpu.VMEM((2, 8, 8, DB), F32),
            pltpu.VMEM((2, 2, 8, DB), BF),
            pltpu.VMEM((2, 2, 8, DB), BF),
            dma((2,)), dma((2, 3)),
            dma((2,)), dma((SEMS[0],)),
            dma((5,)),
            dma((2,)), dma((2, 4)),
            dma((2,)), dma((2, 4)),
            dma((2,)), dma((2, 4)),
            dma((2,)), dma((2, 4)),
            dma((2,)), dma((SEMS[1],)),
            dma((2, 2)), dma((2, 2)),
            dma((2,)), dma((2, 4)),
        ],
        compiler_params=pltpu.CompilerParams(
            collective_id=0, has_side_effects=True, vmem_limit_bytes=53 * 1024 * 1024
        ),
    )(tokens, cotangent, w_gate, w_up, w_down)
    return pl.pallas_call(
        write_out,
        name="write_out",
        out_shape=(
            jax.ShapeDtypeStruct((8, D), BF),
            jax.ShapeDtypeStruct((8, D), BF),
            jax.ShapeDtypeStruct((DB, H), F32),
            jax.ShapeDtypeStruct((DB, H), F32),
            jax.ShapeDtypeStruct((H, DB), F32),
        ),
        in_specs=[vmem] * 3,
        out_specs=(anyw,) * 5,
        scratch_shapes=[pltpu.VMEM((2, 8, D), BF), dma((5,))],
        compiler_params=pltpu.CompilerParams(vmem_limit_bytes=2 * 1024 * 1024),
    )(*held)


def solution(mesh):
    split = Mesh(mesh.devices.reshape(2, 2, 2, 4, 4), DP_TP)
    return jax.shard_map(
        body,
        mesh=split,
        in_specs=(P(DP_TP, None), P(None, TP), P(None, TP), P(TP, None), P(DP_TP, None)),
        out_specs=(P(DP_TP, None), P(DP_TP, None), P(DP, TP), P(DP, TP), P(TP, DP)),
        check_vma=False,
    )
```

```python
import functools

import jax
import jax.numpy as jnp
from jax import lax
from jax.experimental import pallas as pl
from jax.experimental.pallas import tpu as pltpu
from jax.sharding import Mesh
from jax.sharding import PartitionSpec as P

TP = ("yl", "x", "z")
DP = ("yh", "co")
DP_TP = DP + TP
BF = jnp.bfloat16
F32 = jnp.float32

D = 7168
DB = 1792
H = 384
T = 1024
CH = 256
HC = 128

KIDS = {0: ((1, 1), (3, -1)), 1: ((2, 1),), 2: (), 3: ()}
IJ = (
    (0, 0),
    (1, 0), (0, 1), (3, 0), (0, 3),
    (2, 0), (1, 1), (3, 1), (1, 3), (0, 2), (3, 3),
    (2, 1), (1, 2), (3, 2), (2, 3),
    (2, 2),
)
LEAVES = ((3, 3), (3, 2), (0, 3), (0, 2))
REDUCE_SHARED = (LEAVES[:2], LEAVES[:2])
KEPT = tuple(ij for ij in IJ if ij[1] < 2)
OI = {ij: n for n, ij in enumerate(IJ)}


def kernel(
    tok_in, cot_in, wg, wu, wd,
    sgu, sdg, yor,
    tok, cot, yin, big, wgu, wdn, gf, rb, xs, rl, yr, bf, rbb, xsb, rlb, yrb,
    sa, sd, hid, dgu, par, keep, rin, pex, yse, far_out, far_in,
    ysend, yrecv, gsend, grecv, wsem, d1s, d1r, e1s, e1r, e2s, e2r,
    d2s, d2r, rsend, rrecv, fsend, frecv, qsend, qrecv,
):
    yh, co, yl = lax.axis_index("yh"), lax.axis_index("co"), lax.axis_index("yl")
    x, z = lax.axis_index("x"), lax.axis_index("z")
    y = yh * 2 + yl
    f = y * 2 + co
    d = yh * 2 + co

    def ring_dev(g):
        gy = g // 2
        return {"yh": gy // 2, "yl": gy % 2, "co": g % 2}

    def y_dev(k):
        gy = (y + k) % 4
        return {"yh": gy // 2, "yl": gy % 2}

    def xz_dev(c, axis, way):
        s = (1 - 2 * (c % 2)) * way
        o = c // 2
        on_x = (1 - o) if axis == 0 else o
        return {"x": (x + s * on_x + 4) % 4, "z": (z + s * (1 - on_x) + 4) % 4}

    other = {"co": 1 - co}
    pair = {"yl": 1 - yl}

    def ours(n):
        return yl * (1 + n) + (1 - yl) * 3 * n

    def its(n):
        return (1 - yl) * (1 + n) + yl * 3 * n

    def rc(src, dst, ss, rs, dev):
        return pltpu.make_async_remote_copy(
            src_ref=src, dst_ref=dst, send_sem=ss, recv_sem=rs,
            device_id=dev, device_id_type=pl.DeviceIdType.MESH,
        )

    def got(dst, rs):
        rc(dst, dst, rs, rs, other).wait_recv()

    def sent(src, ss):
        rc(src, src, ss, ss, other).wait_send()

    w_copies = (
        pltpu.make_async_copy(wg.at[pl.ds(d * DB, DB), :], wgu.at[:, pl.ds(0, H)], wsem.at[0]),
        pltpu.make_async_copy(wu.at[pl.ds(d * DB, DB), :], wgu.at[:, pl.ds(H, H)], wsem.at[1]),
        pltpu.make_async_copy(wd.at[:, pl.ds(d * DB, DB)], wdn, wsem.at[2]),
    )
    in_copies = (
        pltpu.make_async_copy(tok_in, tok, wsem.at[3]),
        pltpu.make_async_copy(cot_in, cot, wsem.at[4]),
    )
    for cp in in_copies + w_copies:
        cp.start()

    barrier = pltpu.get_barrier_semaphore()
    for dev in ({"x": (x + 1) % 4}, {"x": (x + 3) % 4}, {"z": (z + 1) % 4}, {"z": (z + 3) % 4}):
        pl.semaphore_signal(barrier, inc=1, device_id=dev, device_id_type=pl.DeviceIdType.MESH)
    for k in range(1, 8):
        pl.semaphore_signal(
            barrier, inc=1, device_id=ring_dev((f + k) % 8), device_id_type=pl.DeviceIdType.MESH
        )
    pl.semaphore_wait(barrier, 11)

    for a, src in ((0, tok), (1, cot)):
        in_copies[a].wait()

        @pl.loop(0, 7)
        def _(n):
            k = (n + 1) // 2
            g = ((y + k + (k // 2) * (1 - 2 * (k // 3))) % 4) * 2 + (co + n + 1) % 2
            gd = (g // 4) * 2 + g % 2
            rc(
                src.at[:, pl.ds(pl.multiple_of(gd * DB, 128), DB)], yin.at[a, f],
                ysend.at[a], yrecv.at[a, (k + 1) // 2], ring_dev(g),
            ).start()
    for a, src in ((0, tok), (1, cot)):
        yin[a, f] = src[:, pl.ds(pl.multiple_of(d * DB, 128), DB)]

    def rows(oi, c):
        return pl.ds(pl.multiple_of(oi * 64 + c * 16, 16), 16)

    def sem_of(table, a, oi, c):
        base, n = table[a, oi]
        r = (c - y + 4) % 4
        return base + (0 if n == 1 else (r + 3) // 4 if n == 2 else r - (r // 3) * 2)

    def got_blocks(table, sems, buf, a, oi, which):
        part = "acd".find(which) if which in "acd" and which else 1 if which else 0
        lo, hi = COLOURS[which]
        got(buf.at[a, pl.ds(oi * 64, 16 * (hi - lo))], sems.at[table[a, oi][0] + part])

    def near(n):
        return (y + n + (n // 2) * (1 - 2 * (n // 3))) % 4

    def along_second(a, oi, c):
        i, j = IJ[oi]
        src = big.at[a, rows(oi, c)]

        for kid, way in KIDS[j]:
            to = OI[i, kid]
            rc(src, big.at[a, rows(to, c)], gsend.at[a], grecv.at[sem_of(GATHER_SEM, a, to, c)],
               xz_dev(c, 1, way)).start()

    def assemble(a, c):
        halves = [yin[a, c * 2 + h].astype(F32) for h in range(2)]
        big[a, rows(0, c), :] = jnp.concatenate(halves, axis=0).astype(BF)

    def gather_step(a, oi, which):
        i, j = IJ[oi]
        if oi:
            got_blocks(GATHER_SEM, grecv, big, a, oi, which)
        else:
            for part, (w, count) in enumerate((("a", 1), ("bc", 4), ("bd", 2))):
                if which in w or not which:
                    got(yin.at[a, pl.ds(0, count)], yrecv.at[a, part])

        @pl.loop(*COLOURS[which])
        def _(n):
            c = near(n)
            if oi == 0:
                assemble(a, c)
            src = big.at[a, rows(oi, c)]
            if j == 0:
                for kid, way in KIDS[i]:
                    to = OI[kid, 0]
                    rc(src, big.at[a, rows(to, c)], gsend.at[a], grecv.at[sem_of(GATHER_SEM, a, to, c)],
                       xz_dev(c, 0, way)).start()
            if oi:
                along_second(a, oi, c)

        if oi == 0:
            @pl.loop(*COLOURS[which])
            def _(n):
                along_second(a, oi, near(n))

    mine = HC * co
    theirs = HC - mine

    def half_rows(k, off):
        return pl.ds(pl.multiple_of(k * CH + off, HC), HC)

    part = ((gf, rb, xs, rl, yr), (bf, rbb, xsb, rlb, yrb))

    def product(a, k):
        full = part[a][0]
        left = big.at[a, pl.ds(k * CH, CH)]
        if a == 0:
            if k == 0:
                w_copies[0].wait()
                w_copies[1].wait()

            @pl.loop(0, 3)
            def _(n):
                cols = pl.ds(pl.multiple_of(n * 256, 256), 256)
                full[pl.ds(k * CH, CH), cols] = jnp.dot(
                    left[...], wgu[:, cols], preferred_element_type=F32
                )
        else:
            if k == 0:
                w_copies[2].wait()
            full[pl.ds(k * CH, CH), :] = lax.dot_general(
                left[...], wdn[...], (((1,), (1,)), ((), ())), preferred_element_type=F32
            )
        rc(full.at[half_rows(k, theirs)], part[a][1].at[k], d1s.at[a], d1r.at[a, k], other).start()

    def chip_sum(a, k):
        full, recv, out, relay, _ = part[a]
        got(recv.at[k], d1r.at[a, k])
        s = full[half_rows(k, mine), :] + recv[k]
        full[half_rows(k, mine), :] = s
        out[k] = s.astype(BF)
        for w, way in ((0, 1), (1, -1)):
            rc(out.at[k, pl.ds(w * 64, 64)], relay.at[k, w], e1s.at[a], e1r.at[a, k],
               y_dev(way + 4)).start()

    def relay_on(a, k):
        _, _, _, relay, recv = part[a]
        got(relay.at[k], e1r.at[a, k])
        for w, way in ((0, 1), (1, -1)):
            rc(relay.at[k, w], recv.at[k, pl.ds(w * 64, 64)], e2s.at[a], e2r.at[a, k],
               y_dev(way + 4)).start()

    def total(a, k, cols):
        full, _, _, _, recv = part[a]
        return full[half_rows(k, mine), cols] + recv[k, :, cols].astype(F32)

    def arrived(a, k):
        got(part[a][4].at[k], e2r.at[a, k])

    def forward_act(k):
        arrived(0, k)
        gate = total(0, k, pl.ds(0, H))
        up = total(0, k, pl.ds(H, H))
        sig = 1.0 / (1.0 + jnp.exp(-gate))
        act = gate * sig
        sa[pl.ds(k * HC, HC), :] = act
        sd[pl.ds(k * HC, HC), :] = up * sig * (1.0 + gate * (1.0 - sig))
        hid[half_rows(k, mine), :] = (act * up).astype(BF)
        rc(hid.at[half_rows(k, mine)], hid.at[half_rows(k, mine)], d2s.at[0], d2r.at[0, k], other).start()

    def backward_act(k):
        arrived(1, k)
        back = total(1, k, pl.ds(0, H))
        dgu[half_rows(k, mine), pl.ds(0, H)] = (back * sd[pl.ds(k * HC, HC), :]).astype(BF)
        dgu[half_rows(k, mine), pl.ds(H, H)] = (back * sa[pl.ds(k * HC, HC), :]).astype(BF)
        rc(dgu.at[half_rows(k, mine)], dgu.at[half_rows(k, mine)], d2s.at[1], d2r.at[1, k], other).start()

    def put(a, k, cols, r):
        for n in range(8):
            oi = 8 * k + n
            piece = r[n * 64 : n * 64 + 64]
            if IJ[oi] in KEPT:
                keep[a, pl.ds(KEPT.index(IJ[oi]) * 64, 64), cols] = piece
            else:
                par[a, pl.ds(oi * 64, 64), cols] = piece.astype(BF)

    def mixed_part(k):
        for n in (2 * k, 2 * k + 1):
            got(hid.at[half_rows(n, theirs)], d2r.at[0, n])

        for n in range(7):
            cols = pl.ds(n * 256, 256)
            put(0, k, cols, jnp.dot(
                hid[pl.ds(k * 512, 512), :], wdn[:, cols], preferred_element_type=F32
            ))

    def igrad_part(k):
        for n in (2 * k, 2 * k + 1):
            got(dgu.at[half_rows(n, theirs)], d2r.at[1, n])

        for n in range(7):
            cols = pl.ds(n * 256, 256)
            put(1, k, cols, lax.dot_general(
                dgu[pl.ds(k * 512, 512), :], wgu[cols, :], (((1,), (1,)), ((), ())),
                preferred_element_type=F32,
            ))

    def reduce_step(a, oi, which):
        i, j = IJ[oi]
        kids = [OI[i, kid] for kid, _ in KIDS[j] if (i, kid) not in REDUCE_SHARED[a]]
        if j == 0:
            kids += [OI[kid, 0] for kid, _ in KIDS[i]]
        if oi:
            way = next(w for p in KIDS for q, w in KIDS[p] if q == (j or i))
            axis = 1 if j else 0

        def send(c):
            rc(par.at[a, rows(oi, c)], rin.at[a, rows(oi, c)], rsend.at[a],
               rrecv.at[sem_of(REDUCE_SEM, a, oi, c)], xz_dev(c, axis, -way)).start()

        if which:
            leaf = LEAVES.index((i, j)) if (i, j) in LEAVES else None
        if which == "y":
            @pl.loop(0, 2)
            def _(n):
                rc(par.at[a, rows(oi, its(n))], pex.at[a, leaf, n], qsend.at[a],
                   qrecv.at[a, leaf], pair).start()
            return
        if which == "x":
            got(pex.at[a, leaf], qrecv.at[a, leaf])

            @pl.loop(0, 2)
            def _(n):
                c = ours(n)
                par[a, rows(oi, c), :] = (
                    par[a, rows(oi, c), :].astype(F32) + pex[a, leaf, n].astype(F32)
                ).astype(BF)
                send(c)
            return
        if which == "k":
            got(rin.at[a, pl.ds(oi * 64, 32)], rrecv.at[REDUCE_SEM[a, oi][0]])

            @pl.loop(0, 2)
            def _(n):
                c = ours(n)
                keep[a, rows(KEPT.index(above(oi)), c), :] += rin[a, rows(oi, c), :].astype(F32)
            return

        for kid in kids:
            got_blocks(REDUCE_SEM, rrecv, rin, a, kid, which)

        @pl.loop(*COLOURS[which])
        def _(n):
            c = near(3 - n) if which == "" else near(n)
            if (i, j) in KEPT:
                acc = keep[a, rows(KEPT.index((i, j)), c), :]
                for kid in kids:
                    acc += rin[a, rows(kid, c), :].astype(F32)
                if oi:
                    par[a, rows(oi, c), :] = acc.astype(BF)
                else:
                    for h in range(2):
                        g = c * 2 + h
                        piece = acc[h * 8 : h * 8 + 8]
                        far = c == (y + 2) % 4

                        @pl.when(far)
                        def _():
                            far_out[a, h] = piece.astype(BF)
                            rc(far_out.at[a, h], far_in.at[a, co], fsend.at[a, 1], frecv.at[a, 1],
                               ring_dev(g)).start()

                        @pl.when(jnp.logical_not(far))
                        def _():
                            yse[a, g] = piece

                        @pl.when(jnp.logical_not(far | (g == f)))
                        def _():
                            rc(yse.at[a, g], yor.at[a, f], fsend.at[a, 0], frecv.at[a, 0],
                               ring_dev(g)).start()
            if oi:
                send(c)

    def finish(a):
        yor[a, f] = yse[a, f]
        got(yor.at[a, pl.ds(0, 5)], frecv.at[a, 0])
        got(far_in.at[a], frecv.at[a, 1])
        for h in range(2):
            yor[a, ((y + 2) % 4) * 2 + h] = far_in[a, h].astype(F32)

    def down_piece(n):
        cols = pl.ds(n * 1024, 1024 - 256 * n)
        sdg[:, cols] = lax.dot_general(
            hid[...], big[1, :, cols], (((0,), (0,)), ((), ())), preferred_element_type=F32
        )

    def gate_up_piece(n):
        r = pl.ds(n * 256, 256)
        sgu[r, :] = lax.dot_general(
            big[0, :, r], dgu[...], (((0,), (0,)), ((), ())), preferred_element_type=F32
        )

    def all_sent(a):
        sent(yin.at[a, pl.ds(0, 7)], ysend.at[a])
        sent(big.at[a, pl.ds(0, 15 * 64)], gsend.at[a])
        sent(part[a][1], d1s.at[a])
        sent(part[a][3], e1s.at[a])
        sent(part[a][3], e2s.at[a])
        sent((hid, dgu)[a].at[pl.ds(0, T // 2)], d2s.at[a])
        if a == 0:
            shared = len(REDUCE_SHARED[a])
            sent(pex.at[a, pl.ds(0, shared)], qsend.at[a])
            sent(par.at[a, pl.ds(0, 15 * 64 - 32 * shared)], rsend.at[a])

    steps = {
        "Z": all_sent,
        "T": functools.partial(gather_step, 0),
        "C": functools.partial(gather_step, 1),
        "GU": functools.partial(product, 0),
        "B": functools.partial(product, 1),
        "S": functools.partial(chip_sum, 0),
        "SB": functools.partial(chip_sum, 1),
        "R": functools.partial(relay_on, 0),
        "RB": functools.partial(relay_on, 1),
        "H": forward_act,
        "DB": backward_act,
        "M": mixed_part,
        "I": igrad_part,
        "RM": functools.partial(reduce_step, 0),
        "RI": functools.partial(reduce_step, 1),
        "WD": down_piece,
        "WG": gate_up_piece,
        "FM": finish,
        "FI": finish,
    }
    for word in PROGRAM:
        name, number, which = split_word(word)
        with jax.named_scope(word):
            if name in ("T", "C", "RM", "RI"):
                steps[name](number, which)
            else:
                steps[name](number)

    for a in range(2):
        shared = len(REDUCE_SHARED[a])
        if a:
            sent(pex.at[a, pl.ds(0, shared)], qsend.at[a])
            sent(par.at[a, pl.ds(0, 15 * 64 - 32 * shared)], rsend.at[a])
        sent(yse.at[a, pl.ds(0, 5)], fsend.at[a, 0])
        sent(far_out.at[a], fsend.at[a, 1])


PROGRAM = (
    "T0a", "C0a", "T1a", "T0c", "T0d", "C0b", "T1b", "T3a", "T4b", "T3b", "T4a", "T2b",
    "T2a", "GU0", "S0", "T5", "T6", "T7", "GU1", "T8", "T10", "T9", "R0", "S1",
    "T11", "GU2", "C1", "T14", "T13", "C3", "T12", "C2", "S2", "T15", "GU3", "R1",
    "S3", "C5", "H0", "R2", "C6", "C4", "B0", "H1", "C7", "R3", "M0", "C11",
    "C8", "C9", "C10", "B1", "RM4", "H2", "B2", "C13", "C12", "SB1", "C14", "H3",
    "SB2", "C15", "B3", "SB0", "M1", "RM15", "SB3", "RM12", "RM9", "RB1", "RM14", "WD1",
    "RB2", "RB3", "RB0", "RM11", "RM6", "RM8", "RM10y", "DB2", "DB3", "RM13y", "RM2", "RM5",
    "I1", "RI15", "RI8", "RI13y", "RM10x", "DB1", "RI10y", "RI12", "DB0", "RM13x", "RM1", "RI11",
    "I0", "WG4", "RI14", "WG1", "RI13x", "RM13k", "RM7", "RI10x", "RI6", "WG6", "WD0", "RI5",
    "RI13k", "RI7", "RM10k", "WG0", "RM3", "WG5", "RI10k", "RI9", "WG3", "RI4", "WG2", "RI3a",
    "RI3b", "RI1b", "RM0", "RI2b", "Z0", "Z1", "RI0d", "RI2a", "RI1a", "RI0c", "RI0a", "FM0", "FI1",
)


COLOURS = {"": (0, 4), "a": (0, 1), "b": (1, 4), "c": (1, 3), "d": (3, 4)}


def split_word(word):
    name = word.rstrip("abcdkxy").rstrip("0123456789")
    number = word[len(name):].rstrip("abcdkxy")
    return name, int(number), word[len(name) + len(number):]


def parts_of(name, oi):
    which = {w for a, n, w in map(split_word, PROGRAM) if a == name and n == oi}
    return 3 if "d" in which else 2 if "a" in which else 1


def above(oi):
    i, j = IJ[oi]
    up = next(p for p in KIDS for q, _ in KIDS[p] if q == (j or i))
    return (i, up) if j else (up, 0)


def tables():
    gather, reduce, at = {}, {}, [0, 0]
    for a in range(2):
        for oi in range(1, 16):
            n = parts_of("TC"[a], oi)
            gather[a, oi] = at[0], n
            at[0] += n
            n = 1 if IJ[oi] in REDUCE_SHARED[a] else parts_of(("RM", "RI")[a], OI[above(oi)])
            reduce[a, oi] = at[1], n
            at[1] += n
    return gather, reduce, at


GATHER_SEM, REDUCE_SEM, SEMS = tables()


def write_out(sgu, sdg, yor, mixed, igrad, gg, ug, dg, rows, sem):
    copies = [
        pltpu.make_async_copy(sgu.at[:, pl.ds(0, H)], gg, sem.at[0]),
        pltpu.make_async_copy(sgu.at[:, pl.ds(H, H)], ug, sem.at[1]),
        pltpu.make_async_copy(sdg, dg, sem.at[2]),
    ]
    for cp in copies:
        cp.start()
    for a, out in ((0, mixed), (1, igrad)):
        for b in range(4):
            g = (b // 2) * 4 + b % 2
            rows[a, :, pl.ds(b * DB, DB)] = (yor[a, g] + yor[a, g + 2]).astype(BF)
        copies.append(pltpu.make_async_copy(rows.at[a], out, sem.at[3 + a]))
        copies[-1].start()
    for cp in copies:
        cp.wait()


def body(tokens, w_gate, w_up, w_down, cotangent):
    vmem = pl.BlockSpec(memory_space=pltpu.VMEM)
    anyw = pl.BlockSpec(memory_space=pl.ANY)
    dma = pltpu.SemaphoreType.DMA
    held = pl.pallas_call(
        kernel,
        name="ffn",
        out_shape=(
            pltpu.VMEM((DB, 2 * H), F32),
            pltpu.VMEM((H, DB), F32),
            pltpu.VMEM((2, 8, 8, DB), F32),
        ),
        in_specs=[anyw] * 5,
        out_specs=(vmem, vmem, vmem),
        scratch_shapes=[
            pltpu.VMEM((8, D), BF),
            pltpu.VMEM((8, D), BF),
            pltpu.VMEM((2, 8, 8, DB), BF),
            pltpu.VMEM((2, T, DB), BF),
            pltpu.VMEM((DB, 2 * H), BF),
            pltpu.VMEM((H, DB), BF),
            pltpu.VMEM((T, 2 * H), F32),
            pltpu.VMEM((4, HC, 2 * H), F32),
            pltpu.VMEM((4, HC, 2 * H), BF),
            pltpu.VMEM((4, 2, 64, 2 * H), BF),
            pltpu.VMEM((4, HC, 2 * H), BF),
            pltpu.VMEM((T, H), F32),
            pltpu.VMEM((4, HC, H), F32),
            pltpu.VMEM((4, HC, H), BF),
            pltpu.VMEM((4, 2, 64, H), BF),
            pltpu.VMEM((4, HC, H), BF),
            pltpu.VMEM((T // 2, H), F32),
            pltpu.VMEM((T // 2, H), F32),
            pltpu.VMEM((T, H), BF),
            pltpu.VMEM((T, 2 * H), BF),
            pltpu.VMEM((2, T, DB), BF),
            pltpu.VMEM((2, T // 2, DB), F32),
            pltpu.VMEM((2, T, DB), BF),
            pltpu.VMEM((2, 4, 2, 16, DB), BF),
            pltpu.VMEM((2, 8, 8, DB), F32),
            pltpu.VMEM((2, 2, 8, DB), BF),
            pltpu.VMEM((2, 2, 8, DB), BF),
            dma((2,)), dma((2, 3)),
            dma((2,)), dma((SEMS[0],)),
            dma((5,)),
            dma((2,)), dma((2, 4)),
            dma((2,)), dma((2, 4)),
            dma((2,)), dma((2, 4)),
            dma((2,)), dma((2, 4)),
            dma((2,)), dma((SEMS[1],)),
            dma((2, 2)), dma((2, 2)),
            dma((2,)), dma((2, 4)),
        ],
        compiler_params=pltpu.CompilerParams(
            collective_id=0, has_side_effects=True, vmem_limit_bytes=53 * 1024 * 1024
        ),
    )(tokens, cotangent, w_gate, w_up, w_down)
    return pl.pallas_call(
        write_out,
        name="write_out",
        out_shape=(
            jax.ShapeDtypeStruct((8, D), BF),
            jax.ShapeDtypeStruct((8, D), BF),
            jax.ShapeDtypeStruct((DB, H), F32),
            jax.ShapeDtypeStruct((DB, H), F32),
            jax.ShapeDtypeStruct((H, DB), F32),
        ),
        in_specs=[vmem] * 3,
        out_specs=(anyw,) * 5,
        scratch_shapes=[pltpu.VMEM((2, 8, D), BF), dma((5,))],
        compiler_params=pltpu.CompilerParams(vmem_limit_bytes=2 * 1024 * 1024),
    )(*held)


def solution(mesh):
    split = Mesh(mesh.devices.reshape(2, 2, 2, 4, 4), DP_TP)
    return jax.shard_map(
        body,
        mesh=split,
        in_specs=(P(DP_TP, None), P(None, TP), P(None, TP), P(TP, None), P(DP_TP, None)),
        out_specs=(P(DP_TP, None), P(DP_TP, None), P(DP, TP), P(DP, TP), P(TP, DP)),
        check_vma=False,
    )
```
